128 devices in a mesh: row: 64 (over z, y, x), col: 2 (over core).
Axes of the slice: x: 4, y: 4, z: 4, core: 2. Of those that a mesh axis runs over, the one named last changes fastest.
Arguments:
- node_feat: bfloat16 [524288, 500], P(('row', 'col'))
- w_one: float32 [500, 256], replicated
- w_two: float32 [256, 7], replicated
- send_rows: int32 [512, 128], P(('row', 'col'))
- edge_src: int32 [524288, 6], P(('row', 'col'))
- edge_wt: float32 [524288, 6], P(('row', 'col'))
- labels: int32 [524288], P(('row', 'col'))
- label_mask: int32 [524288], P(('row', 'col'))
Outputs:
- output 1: float32 [], replicated
- output 2: float32 [500, 256], replicated
- output 3: float32 [256, 7], replicated
All inputs are finite; a program needn't handle non-finite values.
Results may differ from the reference program's by a relative error of at most 0.001.
Values are sent between devices in bfloat16 or wider.
A program may use at most 1 GiB of HBM per device.

```python
import jax
import jax.numpy as jnp
from jax import lax

GRID_ROWS = 64
GRID_COLS = 2
NODES_DEV = 4096
HALO_ROWS = 128
DEGREE = 6
FEAT_IN = 500
FEAT_HID = 256
CLASSES = 7
PEERS = 4


def setup_inputs(seed: int = 0) -> dict:
    n_devices = GRID_ROWS * GRID_COLS
    n_nodes = n_devices * NODES_DEV
    key_list = jax.random.split(jax.random.key(seed), 12)
    node_feat = jax.random.normal(key_list[0], (n_nodes, FEAT_IN), jnp.float32).astype(jnp.bfloat16)
    w_one = jax.random.normal(key_list[1], (FEAT_IN, FEAT_HID), jnp.float32) * FEAT_IN ** -0.5
    w_two = jax.random.normal(key_list[2], (FEAT_HID, CLASSES), jnp.float32) * FEAT_HID ** -0.5
    send_rows = jax.random.randint(key_list[3], (n_devices * PEERS, HALO_ROWS), 0, NODES_DEV)
    own_src = jax.random.randint(key_list[4], (n_nodes, DEGREE), 0, NODES_DEV)
    halo_src = jax.random.randint(key_list[5], (n_nodes, DEGREE), NODES_DEV, NODES_DEV + PEERS * HALO_ROWS)
    forced_pos = jax.random.randint(key_list[6], (n_nodes, 1), 0, DEGREE)
    coin_draw = jax.random.randint(key_list[7], (n_nodes, DEGREE), 0, 8)
    is_cut = (coin_draw == 0) | (jnp.arange(DEGREE)[None, :] == forced_pos)
    edge_src = jnp.where(is_cut, halo_src, own_src)
    raw_wt = jax.random.uniform(key_list[8], (n_nodes, DEGREE), jnp.float32, 0.5, 1.5)
    edge_wt = raw_wt * lax.rsqrt(jnp.sum(raw_wt * raw_wt, axis=1, keepdims=True))
    labels = jax.random.randint(key_list[9], (n_nodes,), 0, CLASSES)
    mask_draw = jax.random.randint(key_list[10], (n_nodes,), 0, 2)
    label_mask = jnp.where(jnp.arange(n_nodes) % NODES_DEV == 0, 1, mask_draw)
    return {"node_feat": node_feat, "w_one": w_one, "w_two": w_two, "send_rows": send_rows,
            "edge_src": edge_src, "edge_wt": edge_wt, "labels": labels, "label_mask": label_mask}


def extended_globals(send_rows):
    n_devices = GRID_ROWS * GRID_COLS
    list_table = send_rows.reshape(n_devices, PEERS, HALO_ROWS)
    dev_ids = jnp.arange(n_devices)
    row_id = dev_ids // GRID_COLS
    col_id = dev_ids % GRID_COLS
    peer_dev = jnp.stack([
        row_id * GRID_COLS + (col_id - 1) % GRID_COLS,
        row_id * GRID_COLS + (col_id + 1) % GRID_COLS,
        ((row_id - 1) % GRID_ROWS) * GRID_COLS + col_id,
        ((row_id + 1) % GRID_ROWS) * GRID_COLS + col_id], axis=1)
    back_slot = jnp.array([1, 0, 3, 2])
    halo_rows = peer_dev[:, :, None] * NODES_DEV + list_table[peer_dev, back_slot[None, :], :]
    own_rows = dev_ids[:, None] * NODES_DEV + jnp.arange(NODES_DEV)[None, :]
    return jnp.concatenate([own_rows, halo_rows.reshape(n_devices, PEERS * HALO_ROWS)], axis=1)


def global_src(send_rows, edge_src):
    n_devices = GRID_ROWS * GRID_COLS
    ext_global = extended_globals(send_rows)
    local_src = edge_src.reshape(n_devices, NODES_DEV * DEGREE)
    return jnp.take_along_axis(ext_global, local_src, axis=1).reshape(n_devices * NODES_DEV, DEGREE)


def aggregate(table, gidx, edge_wt):
    def add_edge(total, cols):
        idx_col, wt_col = cols
        return total + wt_col[:, None] * table[idx_col].astype(jnp.float32), None
    start_acc = jnp.zeros((gidx.shape[0], table.shape[1]), jnp.float32)
    result, _ = lax.scan(add_edge, start_acc, (gidx.T, edge_wt.T))
    return result


def scatter_back(grad, gidx, edge_wt):
    def add_edge(total, cols):
        idx_col, wt_col = cols
        return total.at[idx_col].add(wt_col[:, None] * grad), None
    start_acc = jnp.zeros(grad.shape, jnp.float32)
    result, _ = lax.scan(add_edge, start_acc, (gidx.T, edge_wt.T))
    return result


def reference(node_feat, w_one, w_two, send_rows, edge_src, edge_wt, labels, label_mask):
    gidx = global_src(send_rows, edge_src)
    w_one_b = w_one.astype(jnp.bfloat16)
    w_two_b = w_two.astype(jnp.bfloat16)
    z_one = aggregate(node_feat, gidx, edge_wt).astype(jnp.bfloat16)
    h_one = jnp.maximum(jnp.dot(z_one, w_one_b, preferred_element_type=jnp.float32), 0.0).astype(jnp.bfloat16)
    z_two = aggregate(h_one, gidx, edge_wt).astype(jnp.bfloat16)
    logits = jnp.dot(z_two, w_two_b, preferred_element_type=jnp.float32)
    weight = label_mask.astype(jnp.float32)
    label_count = jnp.sum(weight)
    log_norm = jax.nn.logsumexp(logits, axis=1)
    picked = jnp.take_along_axis(logits, labels[:, None], axis=1)[:, 0]
    mean_loss = jnp.sum(weight * (log_norm - picked)) / label_count
    class_prob = jnp.exp(logits - log_norm[:, None])
    onehot = (jnp.arange(CLASSES)[None, :] == labels[:, None]).astype(jnp.float32)
    d_logits = ((class_prob - onehot) * (weight / label_count)[:, None]).astype(jnp.bfloat16)
    grad_two = jnp.dot(z_two.T, d_logits, preferred_element_type=jnp.float32)
    d_z_two = jnp.dot(d_logits, w_two_b.T, preferred_element_type=jnp.float32)
    d_h_one = scatter_back(d_z_two, gidx, edge_wt)
    d_y_one = jnp.where(h_one > 0, d_h_one, 0.0).astype(jnp.bfloat16)
    grad_one = jnp.dot(z_one.T, d_y_one, preferred_element_type=jnp.float32)
    return (mean_loss, grad_one, grad_two)
```

```python
import functools

import jax
import jax.numpy as jnp
from jax import lax
from jax.experimental import pallas as pl
from jax.experimental.pallas import tpu as pltpu
from jax.sharding import PartitionSpec as P

MESH = pl.DeviceIdType.MESH
PEERS = 4
LANES = 128
BLOCK = 256
AR_ROWS = 1024
NT = (((1,), (1,)), ((), ()))
TN = (((0,), (0,)), ((), ()))
F32 = jnp.float32
BF16 = jnp.bfloat16
VMEM = pl.BlockSpec(memory_space=pltpu.VMEM)
SMEM = pl.BlockSpec(memory_space=pltpu.SMEM)


def row_digits(n_rows):
    digits, stride = [], 1
    while stride < n_rows:
        size = min(4, n_rows // stride)
        digits.append((size, stride))
        stride *= size
    return digits


def pieces(value):
    first = value.astype(BF16)
    rest = value - first.astype(F32)
    second = rest.astype(BF16)
    return [first, second, (rest - second.astype(F32)).astype(BF16)]


def iota(shape, dim):
    return lax.broadcasted_iota(jnp.int32, shape, dim)


def block_of_unit(shape):
    return lax.shift_right_logical(iota(shape, 0) * 9363, 16)


def spread_classes(n_class):
    unit = iota((LANES, 8), 0)
    return ((unit - block_of_unit((LANES, 8)) * n_class) == iota((LANES, 8), 1)).astype(F32).astype(BF16)


def block_rows(blk):
    return pl.ds(pl.multiple_of(blk * BLOCK, BLOCK), BLOCK)


def remote(src, dst, send, recv, dev):
    return pltpu.make_async_remote_copy(src_ref=src, dst_ref=dst, send_sem=send, recv_sem=recv,
                                        device_id=dev, device_id_type=MESH)


def finish(copies):
    for copy in copies:
        copy.wait_recv()
    for copy in copies:
        copy.wait_send()


def grid_peers(n_rows, n_cols):
    row, col = lax.axis_index('row'), lax.axis_index('col')
    return [(row, lax.rem(col + n_cols - 1, n_cols)), (row, lax.rem(col + 1, n_cols)),
            (lax.rem(row + n_rows - 1, n_rows), col), (lax.rem(row + 1, n_rows), col)]


def torus_axes(n_rows, n_cols):
    row, col = lax.axis_index('row'), lax.axis_index('col')
    axes = [(n_cols, col, lambda d: (row, lax.rem(col + d, n_cols)))]
    for size, stride in row_digits(n_rows):
        place = lax.rem(row // stride, size)
        axes.append((size, place, functools.partial(
            lambda d, size, stride, place: (row + (lax.rem(place + d, size) - place) * stride, col),
            size=size, stride=stride, place=place)))
    return axes


def meet(devices):
    barrier = pltpu.get_barrier_semaphore()
    for dev in devices:
        pl.semaphore_signal(barrier, inc=1, device_id=dev, device_id_type=MESH)
    pl.semaphore_wait(barrier, len(devices))


def start_exchange(peers, sbuf, rbuf, send_sem, recv_sem):
    copies = [remote(sbuf.at[q], rbuf.at[q ^ 1], send_sem.at[q], recv_sem.at[q ^ 1], peers[q]) for q in range(PEERS)]
    for copy in copies:
        copy.start()
    return copies


def exchange_kernel(n_rows, n_cols, sbuf, rbuf, send_sem, recv_sem):
    peers = grid_peers(n_rows, n_cols)
    meet(peers)
    finish(start_exchange(peers, sbuf, rbuf, send_sem, recv_sem))


def exchange_count_kernel(n_rows, n_cols, sbuf, count, rbuf, total_out, cv, cr, send_sem, recv_sem, c_send, c_recv):
    peers, axes = grid_peers(n_rows, n_cols), torus_axes(n_rows, n_cols)
    meet(peers + [dev(d) for size, _, dev in axes for d in range(1, size)])
    copies = start_exchange(peers, sbuf, rbuf, send_sem, recv_sem)
    for i, (size, _, dev) in enumerate(axes):
        held = count if i == 0 else cv.at[i - 1]
        counts = [remote(held, cr.at[i, d - 1], c_send.at[i, d - 1], c_recv.at[i, d - 1], dev(d))
                  for d in range(1, size)]
        for copy in counts:
            copy.start()
        finish(counts)
        total = held[...]
        for d in range(1, size):
            total = total + cr[i, d - 1]
        cv[i] = total
    total_out[...] = cv[len(axes) - 1]
    finish(copies)


def reduce_kernel(n_rows, n_cols, n_feat, n_class, ar, count, g1_out, g2_out, loss_out, part, gb, rs,
                  r_send, r_recv, g_send, g_recv):
    axes = torus_axes(n_rows, n_cols)
    meet([dev(d) for size, _, dev in axes for d in range(1, size)])
    length, base, spans, at, offset, held = AR_ROWS, 0, [], 0, 0, ar
    for i, (size, place, dev) in enumerate(axes):
        length //= size
        copies = []
        for d in range(1, size):
            there = pl.multiple_of(lax.rem(place + d, size) * length, 8)
            copies.append(remote(held.at[pl.ds(there, length), :], rs.at[pl.ds(at + (d - 1) * length, length), :],
                                 r_send.at[i, d - 1], r_recv.at[i, d - 1], dev(d)))
        for copy in copies:
            copy.start()
        finish(copies)
        total = held[pl.ds(pl.multiple_of(place * length, 8), length), :]
        for d in range(1, size):
            total = total + rs[at + (d - 1) * length:at + d * length, :]
        part[offset:offset + length, :] = total
        held = part.at[pl.ds(offset, length), :]
        base = pl.multiple_of(base + place * length, 8)
        at += (size - 1) * length
        offset += length
        spans.append((base, length))
    gb[pl.ds(base, length), :] = held[...]
    for i in reversed(range(len(axes))):
        size, _, dev = axes[i]
        base, length = spans[i]
        here = gb.at[pl.ds(base, length), :]
        copies = [remote(here, here, g_send.at[i, d - 1], g_recv.at[i, d - 1], dev(d)) for d in range(1, size)]
        for copy in copies:
            copy.start()
        finish(copies)
    half = AR_ROWS // 2
    for j in range(2):
        lanes = slice(j * LANES, (j + 1) * LANES)
        g1_out[:, lanes] = gb[j * half:j * half + n_feat, :]
        g2_out[:, lanes] = gb[j * half + n_feat:j * half + n_feat + n_class, :]
    loss_out[...] = gb[n_feat + n_class:n_feat + n_class + 1, :] / count[0:1, :]


def send_kernel(xt, send_v, msk, sbuf, count):
    n_feat, n_local = xt.shape
    wide = sbuf.shape[1]
    count[...] = jnp.full(count.shape, jnp.sum(msk[...].astype(F32)), F32)
    for q in range(PEERS):
        dst = send_v[q:q + 1, :]

        def pick(blk, total):
            hot = (iota((BLOCK, wide), 0) + blk * BLOCK == dst).astype(F32).astype(BF16)
            return total + lax.dot_general(hot, xt[:, block_rows(blk)], (((0,), (1,)), ((), ())),
                                           preferred_element_type=F32)

        rows = lax.fori_loop(0, n_local // BLOCK, pick, jnp.zeros((wide, n_feat), F32)).astype(BF16)
        sbuf[q, :, 0:n_feat] = rows
        sbuf[q, :, n_feat:] = jnp.zeros((wide, sbuf.shape[2] - n_feat), BF16)


def spread_weights(wt_v, wb):
    def spread(blk, _):
        at = pl.ds(pl.multiple_of(blk * LANES, LANES), LANES)
        for k in range(wt_v.shape[0]):
            wb[k, at, :] = jnp.transpose(jnp.broadcast_to(wt_v[k:k + 1, at], (LANES, LANES)))
        return 0

    lax.fori_loop(0, wt_v.shape[1] // LANES, spread, 0)


def store_halo(table, n_local, rbuf):
    halo = rbuf.shape[1]
    for p in range(PEERS):
        for j in range(rbuf.shape[2] // LANES):
            table[pl.ds((n_local + p * halo) * 4 + j, halo, stride=4), :] = (
                rbuf[p, :, j * LANES:(j + 1) * LANES].astype(F32))


def gather_block(table, parts, src_s, wb, zb, blk):
    degree, n_local, _ = wb.shape

    def some(i, _):
        base = blk * BLOCK + i * 16
        for s in range(16):
            total = None
            for k in range(degree):
                at = pl.multiple_of(src_s[k * n_local + base + s], 4)
                term = table[pl.ds(at, parts), :] * jnp.broadcast_to(wb[k, pl.ds(base + s, 1), :], (parts, LANES))
                total = term if total is None else total + term
            zb[pl.ds(pl.multiple_of((i * 16 + s) * parts, parts), parts), :] = total
        return 0

    lax.fori_loop(0, BLOCK // 16, some, 0)
    return jnp.concatenate([zb[pl.ds(j, BLOCK, stride=parts), :] for j in range(parts)], axis=1).astype(BF16)


def layer_one_kernel(src_s, send_s, xt, wt_v, rbuf, w1, z1, h1, sbuf, tab, tab2, wb, zb, w1b):
    n_feat, n_local = xt.shape
    n_blocks = n_local // BLOCK
    halo = sbuf.shape[1]
    eye = (iota((BLOCK, BLOCK), 0) == iota((BLOCK, BLOCK), 1)).astype(F32).astype(BF16)

    def fill_table(blk, _):
        rows = lax.dot_general(eye, xt[:, block_rows(blk)], NT, preferred_element_type=F32)
        for j in range(4):
            part = rows[:, j * LANES:(j + 1) * LANES]
            if part.shape[1] < LANES:
                part = jnp.concatenate([part, jnp.zeros((BLOCK, LANES - part.shape[1]), F32)], axis=1)
            tab[pl.ds(blk * (4 * BLOCK) + j, BLOCK, stride=4), :] = part
        return 0

    lax.fori_loop(0, n_blocks, fill_table, 0)
    spread_weights(wt_v, wb)
    w1b[...] = jnp.zeros(w1b.shape, BF16)
    w1b[0:n_feat, :] = w1[...].astype(BF16)
    store_halo(tab, n_local, rbuf)

    def layer_one(blk, _):
        rows = block_rows(blk)
        z = gather_block(tab, 4, src_s, wb, zb, blk)
        z1[rows, :] = z
        h = jnp.maximum(jnp.dot(z, w1b[...], preferred_element_type=F32), 0.0).astype(BF16)
        h1[rows, :] = h
        for j in range(2):
            tab2[pl.ds(blk * (2 * BLOCK) + j, BLOCK, stride=2), :] = h[:, j * LANES:(j + 1) * LANES].astype(F32)
        return 0

    lax.fori_loop(0, n_blocks, layer_one, 0)

    for q in range(PEERS):
        def take(i, _):
            for s in range(16):
                r = i * 16 + s
                at = pl.multiple_of(send_s[q * halo + r], 2)
                zb[pl.ds(pl.multiple_of(r * 2, 2), 2), :] = tab2[pl.ds(at, 2), :]
            return 0
        lax.fori_loop(0, halo // 16, take, 0)
        for j in range(2):
            sbuf[q, :, j * LANES:(j + 1) * LANES] = zb[pl.ds(j, halo, stride=2), :].astype(BF16)


def layer_two_kernel(src_s, src_v, wt_v, lab, msk, count, h1, rbuf, w2t, acc, hs, g2t, loss,
                     tab, wb, zb, z2, lg):
    degree, n_local = src_v.shape
    n_class = w2t.shape[0]
    n_blocks = n_local // BLOCK
    halo = rbuf.shape[1]

    def fill_table(blk, _):
        rows = h1[block_rows(blk), :].astype(F32)
        for j in range(2):
            tab[pl.ds(blk * (4 * BLOCK) + j, BLOCK, stride=4), :] = rows[:, j * LANES:(j + 1) * LANES]
        return 0

    lax.fori_loop(0, n_blocks, fill_table, 0)
    spread_weights(wt_v, wb)
    store_halo(tab, n_local, rbuf)
    w2p = jnp.concatenate([w2t[...], jnp.zeros((8 - n_class, w2t.shape[1]), F32)], axis=0).astype(BF16)

    def layer_two(blk, _):
        rows = block_rows(blk)
        z = gather_block(tab, 2, src_s, wb, zb, blk)
        z2[rows, :] = z
        lg[:, rows] = lax.dot_general(w2p, z, NT, preferred_element_type=F32)
        return 0

    lax.fori_loop(0, n_blocks, layer_two, 0)

    logits = lg[...]
    cls = iota(logits.shape, 0)
    real = cls < n_class
    top = jnp.max(jnp.where(real, logits, jnp.finfo(F32).min), axis=0, keepdims=True)
    log_norm = top + jnp.log(jnp.sum(jnp.where(real, jnp.exp(logits - top), 0.0), axis=0, keepdims=True))
    onehot = (cls == lab[...]).astype(F32)
    picked = jnp.sum(onehot * logits, axis=0, keepdims=True)
    weight = msk[...].astype(F32)
    loss[...] = jnp.broadcast_to(jnp.sum(weight * (log_norm - picked), axis=1, keepdims=True), loss.shape)
    prob = jnp.where(real, jnp.exp(logits - log_norm), 0.0)
    lg[...] = (prob - onehot) * (weight / count[0:1, 0:1])

    spread_cls = spread_classes(n_class)
    lc_blk = block_of_unit((LANES, BLOCK))
    slot = iota((BLOCK, BLOCK), 0)
    acc[...] = jnp.zeros(acc.shape, F32)
    g2t[...] = jnp.zeros(g2t.shape, F32)

    def scatter(blk, _):
        cols = block_rows(blk)
        g = lg[:, cols].astype(BF16)
        g2t[...] += jnp.dot(g, z2[cols, :], preferred_element_type=F32)
        tiled = jnp.dot(spread_cls, g, preferred_element_type=F32)
        total = acc[...]
        for k in range(degree):
            src = src_v[k:k + 1, cols]
            left = jnp.where(lax.shift_right_logical(src, 8) == lc_blk, tiled, 0.0).astype(BF16)
            here = (src & (BLOCK - 1)) == slot
            for part in pieces(wt_v[k:k + 1, cols]):
                right = jnp.where(here, part.astype(F32), 0.0).astype(BF16)
                total = total + lax.dot_general(left, right, NT, preferred_element_type=F32)
        acc[...] = total
        return 0

    lax.fori_loop(0, n_blocks, scatter, 0)

    hs[...] = jnp.zeros(hs.shape, F32)
    for p in range(PEERS):
        first = (n_local + p * halo) // BLOCK * n_class
        lane = (n_local + p * halo) % BLOCK
        hs[p, 0:n_class, :] = acc[first:first + n_class, lane:lane + halo]


def weight_grad_kernel(acc, hr, send_v, z1, h1, w2t, g2t, loss, ar):
    n_class = w2t.shape[0]
    n_local = h1.shape[0]
    n_feat = AR_ROWS // 2 - 12
    spread_cls = spread_classes(n_class)
    w2p = jnp.concatenate([w2t[...], jnp.zeros((8 - n_class, w2t.shape[1]), F32)], axis=0).astype(BF16)
    returned = jnp.concatenate([hr[q] for q in range(PEERS)], axis=1)
    dst = send_v[...]
    wide = dst.shape[1]
    dst_blk = lax.shift_right_logical(dst, 8) == block_of_unit((LANES, wide))
    right = ((dst & (BLOCK - 1)) == iota((BLOCK, wide), 0)).astype(F32).astype(BF16)
    total = acc[...]
    for part in pieces(returned):
        tiled = jnp.dot(spread_cls, part, preferred_element_type=F32)
        left = jnp.where(dst_blk, tiled, 0.0).astype(BF16)
        total = total + lax.dot_general(left, right, NT, preferred_element_type=F32)
    turned = jnp.concatenate(pieces(jnp.transpose(total)), axis=1)

    w2_tiled = jnp.dot(spread_cls, w2p, preferred_element_type=F32)
    lc_blk = block_of_unit((LANES, w2t.shape[1]))
    ar[...] = jnp.zeros(ar.shape, F32)
    half = AR_ROWS // 2

    def weight_grad(blk, _):
        rows = block_rows(blk)
        w2_here = jnp.where(lc_blk == blk, w2_tiled, 0.0).astype(BF16)
        dh = jnp.dot(turned, jnp.concatenate([w2_here] * 3, axis=0), preferred_element_type=F32)
        d_one = jnp.where(h1[rows, :].astype(F32) > 0, dh, 0.0).astype(BF16)
        grad = lax.dot_general(z1[rows, :], d_one, TN, preferred_element_type=F32)
        ar[0:half, :] += grad[:, :LANES]
        ar[half:2 * half, :] += grad[:, LANES:]
        return 0

    lax.fori_loop(0, n_local // BLOCK, weight_grad, 0)
    for j in range(2):
        ar[j * half + n_feat:j * half + n_feat + n_class, :] = g2t[0:n_class, j * LANES:(j + 1) * LANES]
    ar[n_feat + n_class:n_feat + n_class + 1, :] = loss[0:1, :]


def call(kernel, name, outs, in_specs, scratch, args, collective=None):
    params = dict(vmem_limit_bytes=60 * 1024 * 1024)
    if collective is not None:
        params = dict(collective_id=collective, has_side_effects=True)
    shapes = tuple(jax.ShapeDtypeStruct(*o) for o in outs)
    return pl.pallas_call(kernel, out_shape=shapes, in_specs=in_specs, out_specs=(VMEM,) * len(outs),
                          scratch_shapes=scratch, compiler_params=pltpu.CompilerParams(**params), name=name)(*args)


def solution(mesh):
    n_rows = mesh.shape['row']
    n_cols = mesh.shape['col']
    grid_axes = ('row', 'col')

    def device_step(node_feat, w_one, w_two, send_rows, edge_src, edge_wt, labels, label_mask):
        n_local, n_feat = node_feat.shape
        hidden, n_class = w_two.shape
        halo = send_rows.shape[1]
        degree = edge_src.shape[1]
        ext = n_local + PEERS * halo
        sizes = [n_cols] + [s for s, _ in row_digits(n_rows)]
        n_axes = len(sizes)
        dma, vm = pltpu.SemaphoreType.DMA, pltpu.VMEM
        feat_pad = 4 * LANES
        xt, src_v, wt_v, w2t = node_feat.T, edge_src.T, edge_wt.T, w_two.T
        src_s = (src_v * 4).reshape(-1)
        lab, msk = labels.reshape(1, -1), label_mask.reshape(1, -1)

        sbuf, count = call(send_kernel, 'send', [((PEERS, halo, feat_pad), BF16), ((8, LANES), F32)],
                           [VMEM] * 3, [], (xt, send_rows, msk))
        rbuf, count = call(
            functools.partial(exchange_count_kernel, n_rows, n_cols), 'exchange_count',
            [((PEERS, halo, feat_pad), BF16), ((8, LANES), F32)], [VMEM] * 2,
            [vm((n_axes, 8, LANES), F32), vm((n_axes, 3, 8, LANES), F32),
             dma((PEERS,)), dma((PEERS,)), dma((n_axes, 3)), dma((n_axes, 3))], (sbuf, count), 0)
        z1, h1, sbuf2 = call(
            layer_one_kernel, 'layer_one',
            [((n_local, feat_pad), BF16), ((n_local, hidden), BF16), ((PEERS, halo, hidden), BF16)],
            [SMEM] * 2 + [VMEM] * 4,
            [vm((ext * 4, LANES), F32), vm((n_local * 2, LANES), F32), vm((degree, n_local, LANES), F32),
             vm((BLOCK * 4, LANES), F32), vm((feat_pad, hidden), BF16)],
            (src_s, (send_rows * 2).reshape(-1), xt, wt_v, rbuf, w_one))
        rbuf2, = call(functools.partial(exchange_kernel, n_rows, n_cols), 'exchange_hidden',
                      [((PEERS, halo, hidden), BF16)], [VMEM], [dma((PEERS,)), dma((PEERS,))], (sbuf2,), 1)
        acc, hs, g2t, loss = call(
            layer_two_kernel, 'layer_two',
            [((LANES, BLOCK), F32), ((PEERS, 8, halo), F32), ((8, hidden), F32), ((8, LANES), F32)],
            [SMEM] + [VMEM] * 8,
            [vm((ext * 4, LANES), F32), vm((degree, n_local, LANES), F32), vm((BLOCK * 2, LANES), F32),
             vm((n_local, hidden), BF16), vm((8, n_local), F32)],
            (src_s, src_v, wt_v, lab, msk, count, h1, rbuf2, w2t))
        hr, = call(functools.partial(exchange_kernel, n_rows, n_cols), 'exchange_grad',
                   [((PEERS, 8, halo), F32)], [VMEM], [dma((PEERS,)), dma((PEERS,))], (hs,), 2)
        ar, = call(weight_grad_kernel, 'weight_grad', [((AR_ROWS, LANES), F32)], [VMEM] * 8, [],
                   (acc, hr, send_rows.reshape(1, -1), z1, h1, w2t, g2t, loss))
        part_rows, rs_rows, left = 0, 0, AR_ROWS
        for size in sizes:
            left //= size
            part_rows += left
            rs_rows += (size - 1) * left
        g1, g2, total = call(
            functools.partial(reduce_kernel, n_rows, n_cols, n_feat, n_class), 'reduce',
            [((n_feat, hidden), F32), ((n_class, hidden), F32), ((1, LANES), F32)], [VMEM] * 2,
            [vm((part_rows, LANES), F32), vm((AR_ROWS, LANES), F32), vm((rs_rows, LANES), F32),
             dma((n_axes, 3)), dma((n_axes, 3)), dma((n_axes, 3)), dma((n_axes, 3))], (ar, count), 3)
        return total[0, 0], g1, g2.T

    rows_spec = P(grid_axes, None)
    vec_spec = P(grid_axes)
    return jax.shard_map(device_step, mesh=mesh,
                         in_specs=(rows_spec, P(), P(), rows_spec, rows_spec, rows_spec, vec_spec, vec_spec),
                         out_specs=(P(), P(), P()), check_vma=False)
```

```python
import functools

import jax
import jax.numpy as jnp
from jax import lax
from jax.experimental import pallas as pl
from jax.experimental.pallas import tpu as pltpu
from jax.sharding import PartitionSpec as P

MESH = pl.DeviceIdType.MESH
PEERS = 4
LANES = 128
BLOCK = 256
AR_ROWS = 1024
NT = (((1,), (1,)), ((), ()))
TN = (((0,), (0,)), ((), ()))
F32 = jnp.float32
BF16 = jnp.bfloat16
VMEM = pl.BlockSpec(memory_space=pltpu.VMEM)
SMEM = pl.BlockSpec(memory_space=pltpu.SMEM)
ANY = pl.BlockSpec(memory_space=pl.ANY)


def row_digits(n_rows):
    digits, stride = [], 1
    while stride < n_rows:
        size = min(4, n_rows // stride)
        digits.append((size, stride))
        stride *= size
    return digits


def pieces(value):
    first = value.astype(BF16)
    rest = value - first.astype(F32)
    second = rest.astype(BF16)
    return [first, second, (rest - second.astype(F32)).astype(BF16)]


def iota(shape, dim):
    return lax.broadcasted_iota(jnp.int32, shape, dim)


def block_of_unit(shape):
    return lax.shift_right_logical(iota(shape, 0) * 9363, 16)


def spread_classes(n_class):
    unit = iota((LANES, 8), 0)
    return ((unit - block_of_unit((LANES, 8)) * n_class) == iota((LANES, 8), 1)).astype(F32).astype(BF16)


def block_rows(blk):
    return pl.ds(pl.multiple_of(blk * BLOCK, BLOCK), BLOCK)


def remote(src, dst, send, recv, dev):
    return pltpu.make_async_remote_copy(src_ref=src, dst_ref=dst, send_sem=send, recv_sem=recv,
                                        device_id=dev, device_id_type=MESH)


def finish(copies):
    for copy in copies:
        copy.wait_recv()
    for copy in copies:
        copy.wait_send()


def grid_peers(n_rows, n_cols):
    row, col = lax.axis_index('row'), lax.axis_index('col')
    return [(row, lax.rem(col + n_cols - 1, n_cols)), (row, lax.rem(col + 1, n_cols)),
            (lax.rem(row + n_rows - 1, n_rows), col), (lax.rem(row + 1, n_rows), col)]


def torus_axes(n_rows, n_cols):
    row, col = lax.axis_index('row'), lax.axis_index('col')
    axes = [(n_cols, col, lambda d: (row, lax.rem(col + d, n_cols)))]
    for size, stride in row_digits(n_rows):
        place = lax.rem(row // stride, size)
        axes.append((size, place, functools.partial(
            lambda d, size, stride, place: (row + (lax.rem(place + d, size) - place) * stride, col),
            size=size, stride=stride, place=place)))
    return axes


def arrive(devices):
    for dev in devices:
        pl.semaphore_signal(pltpu.get_barrier_semaphore(), inc=1, device_id=dev, device_id_type=MESH)


def meet(devices):
    pl.semaphore_wait(pltpu.get_barrier_semaphore(), len(devices))


def start_exchange(peers, sbuf, rbuf, send_sem, recv_sem):
    copies = [remote(sbuf.at[q], rbuf.at[q ^ 1], send_sem.at[q], recv_sem.at[q ^ 1], peers[q]) for q in range(PEERS)]
    for copy in copies:
        copy.start()
    return copies


def axis_devices(axes):
    return [dev(d) for size, _, dev in axes for d in range(1, size)]


def exchange_kernel(n_rows, n_cols, sbuf, rbuf, send_sem, recv_sem):
    peers = grid_peers(n_rows, n_cols)
    arrive(peers)
    meet(peers)
    finish(start_exchange(peers, sbuf, rbuf, send_sem, recv_sem))


def first_kernel(n_rows, n_cols, xt, send_v, src_v, msk, rbuf, total_out, src4, sbuf, count, cv, cr,
                 send_sem, recv_sem, c_send, c_recv):
    peers, axes = grid_peers(n_rows, n_cols), torus_axes(n_rows, n_cols)
    everyone = peers + axis_devices(axes)
    arrive(everyone)
    n_feat, n_local = xt.shape
    halo = sbuf.shape[1]
    count[...] = jnp.full(count.shape, jnp.sum(msk[...].astype(F32)), F32)
    src4[...] = src_v[...] * 4
    wanted = [jnp.transpose(jnp.broadcast_to(send_v[q:q + 1, :], (LANES, halo))) for q in range(PEERS)]
    wanted = jnp.concatenate([jnp.concatenate(wanted, axis=0)] * (BLOCK // LANES), axis=1)
    place = iota(wanted.shape, 1)

    def pick(blk, total):
        hot = (place == wanted - blk * BLOCK).astype(F32).astype(BF16)
        return total + lax.dot_general(hot, xt[:, block_rows(blk)], NT, preferred_element_type=F32)

    rows = lax.fori_loop(0, n_local // BLOCK, pick, jnp.zeros((PEERS * halo, n_feat), F32)).astype(BF16)
    for q in range(PEERS):
        sbuf[q, :, 0:n_feat] = rows[q * halo:(q + 1) * halo, :]
        sbuf[q, :, n_feat:] = jnp.zeros((halo, sbuf.shape[2] - n_feat), BF16)
    meet(everyone)
    copies = start_exchange(peers, sbuf, rbuf, send_sem, recv_sem)
    for i, (size, _, dev) in enumerate(axes):
        held = count if i == 0 else cv.at[i - 1]
        counts = [remote(held, cr.at[i, d - 1], c_send.at[i, d - 1], c_recv.at[i, d - 1], dev(d))
                  for d in range(1, size)]
        for copy in counts:
            copy.start()
        finish(counts)
        total = held[...]
        for d in range(1, size):
            total = total + cr[i, d - 1]
        cv[i] = total
    total_out[...] = cv[len(axes) - 1]
    finish(copies)


def reduce_over_devices(axes, ar, part, gb, rs, r_send, r_recv, g_send, g_recv):
    length, base, spans, at, offset, held = AR_ROWS, 0, [], 0, 0, ar
    for i, (size, place, dev) in enumerate(axes):
        length //= size
        copies = []
        for d in range(1, size):
            there = pl.multiple_of(lax.rem(place + d, size) * length, 8)
            copies.append(remote(held.at[pl.ds(there, length), :], rs.at[pl.ds(at + (d - 1) * length, length), :],
                                 r_send.at[i, d - 1], r_recv.at[i, d - 1], dev(d)))
        for copy in copies:
            copy.start()
        finish(copies)
        total = held[pl.ds(pl.multiple_of(place * length, 8), length), :]
        for d in range(1, size):
            total = total + rs[at + (d - 1) * length:at + d * length, :]
        part[offset:offset + length, :] = total
        held = part.at[pl.ds(offset, length), :]
        base = pl.multiple_of(base + place * length, 8)
        at += (size - 1) * length
        offset += length
        spans.append((base, length))
    gb[pl.ds(base, length), :] = held[...]
    for i in reversed(range(len(axes))):
        size, _, dev = axes[i]
        base, length = spans[i]
        here = gb.at[pl.ds(base, length), :]
        copies = [remote(here, here, g_send.at[i, d - 1], g_recv.at[i, d - 1], dev(d)) for d in range(1, size)]
        for copy in copies:
            copy.start()
        finish(copies)


def turn_weights(wt_v, wcol):
    degree, n_local = wt_v.shape

    def turn(blk, _):
        at = pl.ds(pl.multiple_of(blk * LANES, LANES), LANES)
        wcol[at, :] = jnp.transpose(jnp.concatenate([wt_v[:, at], jnp.zeros((8 - degree, LANES), F32)], axis=0))
        return 0

    lax.fori_loop(0, n_local // LANES, turn, 0)


def store_halo(table, n_local, rbuf):
    halo = rbuf.shape[1]
    for p in range(PEERS):
        for j in range(rbuf.shape[2] // LANES):
            table[pl.ds((n_local + p * halo) * 4 + j, halo, stride=4), :] = (
                rbuf[p, :, j * LANES:(j + 1) * LANES].astype(F32))


GROUP = 16


def spread_weights(wcol, spread, first):
    some = wcol[pl.ds(pl.multiple_of(first, GROUP), GROUP), :]
    for k in range(spread.shape[0]):
        spread[k] = jnp.broadcast_to(some[:, k:k + 1], (GROUP, LANES))


def gather_block(table, parts, src_s, wcol, spreads, zb, blk):
    degree, n_local = src_s.shape

    def some(i, _):
        for half in range(2):
            local = i * (2 * GROUP) + half * GROUP
            base = blk * BLOCK + local
            for s in range(GROUP):
                total = None
                for k in range(degree):
                    at = pl.multiple_of(src_s[k, base + s], 4)
                    weight = jnp.broadcast_to(spreads[half][k, s:s + 1, :], (parts, LANES))
                    term = table[pl.ds(at, parts), :] * weight
                    total = term if total is None else total + term
                zb[pl.ds(pl.multiple_of((local + s) * parts, parts), parts), :] = total
            spread_weights(wcol, spreads[1 - half], jnp.minimum(base + GROUP, n_local - GROUP) if half else base + GROUP)
        return 0

    lax.fori_loop(0, BLOCK // (2 * GROUP), some, 0)
    return jnp.concatenate([zb[pl.ds(j, BLOCK, stride=parts), :] for j in range(parts)], axis=1).astype(BF16)


def layer_one_kernel(src4, send_s, xt, wt_v, rbuf, w1, z1, h1, sbuf,
                     src_s, tab, tab2, wcol, spread_a, spread_b, zb, w1b, z1_v, h1_v, sem):
    n_feat, n_local = xt.shape
    n_blocks = n_local // BLOCK
    halo = sbuf.shape[1]
    indices = pltpu.make_async_copy(src4, src_s, sem.at[0])
    indices.start()
    eye = (iota((BLOCK, BLOCK), 0) == iota((BLOCK, BLOCK), 1)).astype(F32).astype(BF16)

    def fill_table(blk, _):
        rows = lax.dot_general(eye, xt[:, block_rows(blk)], NT, preferred_element_type=F32)
        for j in range(4):
            part = rows[:, j * LANES:(j + 1) * LANES]
            if part.shape[1] < LANES:
                part = jnp.concatenate([part, jnp.zeros((BLOCK, LANES - part.shape[1]), F32)], axis=1)
            tab[pl.ds(blk * (4 * BLOCK) + j, BLOCK, stride=4), :] = part
        return 0

    lax.fori_loop(0, n_blocks, fill_table, 0)
    turn_weights(wt_v, wcol)
    w1b[...] = jnp.zeros(w1b.shape, BF16)
    w1b[0:n_feat, :] = w1[...].astype(BF16)
    store_halo(tab, n_local, rbuf)
    spread_weights(wcol, spread_a, 0)
    indices.wait()

    def layer_one(blk, _):
        rows = block_rows(blk)
        z = gather_block(tab, 4, src_s, wcol, (spread_a, spread_b), zb, blk)
        z1_v[rows, :] = z
        h = jnp.maximum(jnp.dot(z, w1b[...], preferred_element_type=F32), 0.0).astype(BF16)
        h1_v[rows, :] = h
        pltpu.make_async_copy(z1_v.at[rows, :], z1.at[rows, :], sem.at[1]).start()
        pltpu.make_async_copy(h1_v.at[rows, :], h1.at[rows, :], sem.at[2]).start()
        for j in range(2):
            tab2[pl.ds(blk * (2 * BLOCK) + j, BLOCK, stride=2), :] = h[:, j * LANES:(j + 1) * LANES].astype(F32)
        return 0

    lax.fori_loop(0, n_blocks, layer_one, 0)

    for q in range(PEERS):
        def take(i, _):
            for s in range(16):
                r = i * 16 + s
                at = pl.multiple_of(send_s[q, r] * 2, 2)
                zb[pl.ds(pl.multiple_of(r * 2, 2), 2), :] = tab2[pl.ds(at, 2), :]
            return 0
        lax.fori_loop(0, halo // 16, take, 0)
        for j in range(2):
            sbuf[q, :, j * LANES:(j + 1) * LANES] = zb[pl.ds(j, halo, stride=2), :].astype(BF16)
    pltpu.make_async_copy(z1_v, z1, sem.at[1]).wait()
    pltpu.make_async_copy(h1_v, h1, sem.at[2]).wait()


def layer_two_kernel(src4, wt_v, h1, rbuf, w2t, z2, lg, src_s, tab, wcol, spread_a, spread_b, zb, sem):
    n_class = w2t.shape[0]
    n_local = h1.shape[0]
    n_blocks = n_local // BLOCK
    indices = pltpu.make_async_copy(src4, src_s, sem)
    indices.start()

    def fill_table(blk, _):
        rows = h1[block_rows(blk), :].astype(F32)
        for j in range(2):
            tab[pl.ds(blk * (4 * BLOCK) + j, BLOCK, stride=4), :] = rows[:, j * LANES:(j + 1) * LANES]
        return 0

    lax.fori_loop(0, n_blocks, fill_table, 0)
    turn_weights(wt_v, wcol)
    store_halo(tab, n_local, rbuf)
    spread_weights(wcol, spread_a, 0)
    w2p = jnp.concatenate([w2t[...], jnp.zeros((8 - n_class, w2t.shape[1]), F32)], axis=0).astype(BF16)
    indices.wait()

    def layer_two(blk, _):
        rows = block_rows(blk)
        z = gather_block(tab, 2, src_s, wcol, (spread_a, spread_b), zb, blk)
        z2[rows, :] = z
        lg[:, rows] = lax.dot_general(w2p, z, NT, preferred_element_type=F32)
        return 0

    lax.fori_loop(0, n_blocks, layer_two, 0)


def last_kernel(n_rows, n_cols, n_feat, src_v, wt_v, lab, msk, count, logit, z2, w2t, send_v, z1, h1,
                g1_out, g2_out, loss_out, z1_v, h1_v, lg, acc, g2t, hs, hr, ar, part_sum, gb, rs,
                sem, send_sem, recv_sem, r_send, r_recv, g_send, g_recv):
    peers, axes = grid_peers(n_rows, n_cols), torus_axes(n_rows, n_cols)
    everyone = peers + axis_devices(axes)
    arrive(everyone)
    z1_load = pltpu.make_async_copy(z1, z1_v, sem.at[0])
    h1_load = pltpu.make_async_copy(h1, h1_v, sem.at[1])
    z1_load.start()
    h1_load.start()
    degree, n_local = src_v.shape
    n_class = w2t.shape[0]
    n_blocks = n_local // BLOCK
    halo = hs.shape[2]
    half = AR_ROWS // 2

    logits = logit[...]
    cls = iota(logits.shape, 0)
    real = cls < n_class
    top = jnp.max(jnp.where(real, logits, jnp.finfo(F32).min), axis=0, keepdims=True)
    log_norm = top + jnp.log(jnp.sum(jnp.where(real, jnp.exp(logits - top), 0.0), axis=0, keepdims=True))
    onehot = (cls == lab[...]).astype(F32)
    picked = jnp.sum(onehot * logits, axis=0, keepdims=True)
    weight = msk[...].astype(F32)
    loss_sum = jnp.sum(weight * (log_norm - picked), axis=1, keepdims=True)
    prob = jnp.where(real, jnp.exp(logits - log_norm), 0.0)
    lg[...] = (prob - onehot) * (weight / count[0:1, 0:1])

    spread_cls = spread_classes(n_class)
    lc_blk = block_of_unit((LANES, BLOCK))
    slot = iota((BLOCK, BLOCK), 0)
    acc[...] = jnp.zeros(acc.shape, F32)
    g2t[...] = jnp.zeros(g2t.shape, F32)

    def scatter(blk, _):
        cols = block_rows(blk)
        g = lg[:, cols].astype(BF16)
        g2t[...] += jnp.dot(g, z2[cols, :], preferred_element_type=F32)
        tiled = jnp.dot(spread_cls, g, preferred_element_type=F32)
        total = acc[...]
        for k in range(degree):
            src = src_v[k:k + 1, cols]
            left = jnp.where(lax.shift_right_logical(src, 8) == lc_blk, tiled, 0.0).astype(BF16)
            here = (src & (BLOCK - 1)) == slot
            for part in pieces(wt_v[k:k + 1, cols]):
                right = jnp.where(here, part.astype(F32), 0.0).astype(BF16)
                total = total + lax.dot_general(left, right, NT, preferred_element_type=F32)
        acc[...] = total
        return 0

    lax.fori_loop(0, n_blocks, scatter, 0)

    hs[...] = jnp.zeros(hs.shape, F32)
    for p in range(PEERS):
        first = (n_local + p * halo) // BLOCK * n_class
        lane = (n_local + p * halo) % BLOCK
        hs[p, 0:n_class, :] = acc[first:first + n_class, lane:lane + halo]
    meet(everyone)
    copies = start_exchange(peers, hs, hr, send_sem, recv_sem)

    w2p = jnp.concatenate([w2t[...], jnp.zeros((8 - n_class, w2t.shape[1]), F32)], axis=0).astype(BF16)
    w2_tiled = jnp.dot(spread_cls, w2p, preferred_element_type=F32)
    ar[...] = jnp.zeros(ar.shape, F32)
    dst = send_v[...]
    wide = dst.shape[1]
    dst_blk = lax.shift_right_logical(dst, 8) == block_of_unit((LANES, wide))
    right = ((dst & (BLOCK - 1)) == iota((BLOCK, wide), 0)).astype(F32).astype(BF16)
    z1_load.wait()
    h1_load.wait()
    finish(copies)

    total = acc[...]
    returned = jnp.concatenate([hr[q] for q in range(PEERS)], axis=1)
    for part in pieces(returned):
        tiled = jnp.dot(spread_cls, part, preferred_element_type=F32)
        left = jnp.where(dst_blk, tiled, 0.0).astype(BF16)
        total = total + lax.dot_general(left, right, NT, preferred_element_type=F32)
    turned = jnp.concatenate(pieces(jnp.transpose(total)), axis=1)

    def weight_grad(blk, _):
        rows = block_rows(blk)
        w2_here = jnp.where(lc_blk == blk, w2_tiled, 0.0).astype(BF16)
        dh = jnp.dot(turned, jnp.concatenate([w2_here] * 3, axis=0), preferred_element_type=F32)
        d_one = jnp.where(h1_v[rows, :].astype(F32) > 0, dh, 0.0).astype(BF16)
        grad = lax.dot_general(z1_v[rows, :], d_one, TN, preferred_element_type=F32)
        ar[0:half, :] += grad[:, :LANES]
        ar[half:2 * half, :] += grad[:, LANES:]
        return 0

    lax.fori_loop(0, n_blocks, weight_grad, 0)
    for j in range(2):
        ar[j * half + n_feat:j * half + n_feat + n_class, :] = g2t[0:n_class, j * LANES:(j + 1) * LANES]
    ar[n_feat + n_class:n_feat + n_class + 1, :] = jnp.broadcast_to(loss_sum, (1, LANES))

    reduce_over_devices(axes, ar, part_sum, gb, rs, r_send, r_recv, g_send, g_recv)
    for j in range(2):
        lanes = slice(j * LANES, (j + 1) * LANES)
        g1_out[:, lanes] = gb[j * half:j * half + n_feat, :]
        g2_out[:, lanes] = gb[j * half + n_feat:j * half + n_feat + n_class, :]
    loss_out[...] = gb[n_feat + n_class:n_feat + n_class + 1, :] / count[0:1, :]


def call(kernel, name, outs, in_specs, out_specs, scratch, args, collective=None):
    params = dict(vmem_limit_bytes=60 * 1024 * 1024)
    if collective is not None:
        params.update(collective_id=collective, has_side_effects=True)
    shapes = tuple(jax.ShapeDtypeStruct(*o) for o in outs)
    return pl.pallas_call(kernel, out_shape=shapes, in_specs=in_specs, out_specs=tuple(out_specs),
                          scratch_shapes=scratch, compiler_params=pltpu.CompilerParams(**params), name=name)(*args)


def solution(mesh):
    n_rows = mesh.shape['row']
    n_cols = mesh.shape['col']
    grid_axes = ('row', 'col')

    def device_step(node_feat, w_one, w_two, send_rows, edge_src, edge_wt, labels, label_mask):
        n_local, n_feat = node_feat.shape
        hidden, n_class = w_two.shape
        halo = send_rows.shape[1]
        degree = edge_src.shape[1]
        ext = n_local + PEERS * halo
        sizes = [n_cols] + [s for s, _ in row_digits(n_rows)]
        n_axes = len(sizes)
        dma, vm = pltpu.SemaphoreType.DMA, pltpu.VMEM
        feat_pad = 4 * LANES
        xt, src_v, wt_v, w2t = node_feat.T, edge_src.T, edge_wt.T, w_two.T
        lab, msk = labels.reshape(1, -1), label_mask.reshape(1, -1)
        spreads = [vm((degree, GROUP, LANES), F32)] * 2

        rbuf, count, src4 = call(
            functools.partial(first_kernel, n_rows, n_cols), 'first',
            [((PEERS, halo, feat_pad), BF16), ((8, LANES), F32), ((degree, n_local), jnp.int32)],
            [VMEM] * 4, [VMEM] * 3,
            [vm((PEERS, halo, feat_pad), BF16), vm((8, LANES), F32),
             vm((n_axes, 8, LANES), F32), vm((n_axes, 3, 8, LANES), F32),
             dma((PEERS,)), dma((PEERS,)), dma((n_axes, 3)), dma((n_axes, 3))], (xt, send_rows, src_v, msk), 0)
        z1, h1, sbuf2 = call(
            layer_one_kernel, 'layer_one',
            [((n_local, feat_pad), BF16), ((n_local, hidden), BF16), ((PEERS, halo, hidden), BF16)],
            [ANY, SMEM] + [VMEM] * 4, [ANY, ANY, VMEM],
            [pltpu.SMEM((degree, n_local), jnp.int32), vm((ext * 4, LANES), F32), vm((n_local * 2, LANES), F32),
             vm((n_local, 8), F32), *spreads, vm((BLOCK * 4, LANES), F32), vm((feat_pad, hidden), BF16),
             vm((n_local, feat_pad), BF16), vm((n_local, hidden), BF16), dma((3,))],
            (src4, send_rows, xt, wt_v, rbuf, w_one))
        rbuf2, = call(functools.partial(exchange_kernel, n_rows, n_cols), 'exchange_hidden',
                      [((PEERS, halo, hidden), BF16)], [VMEM], [VMEM], [dma((PEERS,)), dma((PEERS,))], (sbuf2,), 1)
        z2, logit = call(
            layer_two_kernel, 'layer_two', [((n_local, hidden), BF16), ((8, n_local), F32)],
            [ANY] + [VMEM] * 4, [VMEM] * 2,
            [pltpu.SMEM((degree, n_local), jnp.int32), vm((ext * 4, LANES), F32), vm((n_local, 8), F32), *spreads,
             vm((BLOCK * 2, LANES), F32), dma(())],
            (src4, wt_v, h1, rbuf2, w2t))
        part_rows, rs_rows, left = 0, 0, AR_ROWS
        for size in sizes:
            left //= size
            part_rows += left
            rs_rows += (size - 1) * left
        g1, g2, total = call(
            functools.partial(last_kernel, n_rows, n_cols, n_feat), 'last',
            [((n_feat, hidden), F32), ((n_class, hidden), F32), ((1, LANES), F32)],
            [VMEM] * 9 + [ANY] * 2, [VMEM] * 3,
            [vm((n_local, feat_pad), BF16), vm((n_local, hidden), BF16), vm((8, n_local), F32),
             vm((LANES, BLOCK), F32), vm((8, hidden), F32), vm((PEERS, 8, halo), F32), vm((PEERS, 8, halo), F32),
             vm((AR_ROWS, LANES), F32), vm((part_rows, LANES), F32), vm((AR_ROWS, LANES), F32),
             vm((rs_rows, LANES), F32), dma((2,)), dma((PEERS,)), dma((PEERS,)),
             dma((n_axes, 3)), dma((n_axes, 3)), dma((n_axes, 3)), dma((n_axes, 3))],
            (src_v, wt_v, lab, msk, count, logit, z2, w2t, send_rows.reshape(1, -1), z1, h1), 2)
        return total[0, 0], g1, g2.T

    rows_spec = P(grid_axes, None)
    vec_spec = P(grid_axes)
    return jax.shard_map(device_step, mesh=mesh,
                         in_specs=(rows_spec, P(), P(), rows_spec, rows_spec, rows_spec, vec_spec, vec_spec),
                         out_specs=(P(), P(), P()), check_vma=False)
```

```python
import functools

import jax
import jax.numpy as jnp
from jax import lax
from jax.experimental import pallas as pl
from jax.experimental.pallas import tpu as pltpu
from jax.sharding import PartitionSpec as P

MESH = pl.DeviceIdType.MESH
PEERS = 4
LANES = 128
BLOCK = 256
AR_ROWS = 1024
NT = (((1,), (1,)), ((), ()))
TN = (((0,), (0,)), ((), ()))
F32 = jnp.float32
BF16 = jnp.bfloat16
VMEM = pl.BlockSpec(memory_space=pltpu.VMEM)
SMEM = pl.BlockSpec(memory_space=pltpu.SMEM)
ANY = pl.BlockSpec(memory_space=pl.ANY)


def row_digits(n_rows):
    digits, stride = [], 1
    while stride < n_rows:
        size = min(4, n_rows // stride)
        digits.append((size, stride))
        stride *= size
    return digits


def pieces(value):
    first = value.astype(BF16)
    rest = value - first.astype(F32)
    second = rest.astype(BF16)
    return [first, second, (rest - second.astype(F32)).astype(BF16)]


def iota(shape, dim):
    return lax.broadcasted_iota(jnp.int32, shape, dim)


def block_of_unit(shape):
    return lax.shift_right_logical(iota(shape, 0) * 9363, 16)


def spread_classes(n_class):
    unit = iota((LANES, 8), 0)
    return ((unit - block_of_unit((LANES, 8)) * n_class) == iota((LANES, 8), 1)).astype(F32).astype(BF16)


def block_rows(blk):
    return pl.ds(pl.multiple_of(blk * BLOCK, BLOCK), BLOCK)


def remote(src, dst, send, recv, dev):
    return pltpu.make_async_remote_copy(src_ref=src, dst_ref=dst, send_sem=send, recv_sem=recv,
                                        device_id=dev, device_id_type=MESH)


def finish(copies):
    for copy in copies:
        copy.wait_recv()
    for copy in copies:
        copy.wait_send()


def grid_peers(n_rows, n_cols):
    row, col = lax.axis_index('row'), lax.axis_index('col')
    return [(row, lax.rem(col + n_cols - 1, n_cols)), (row, lax.rem(col + 1, n_cols)),
            (lax.rem(row + n_rows - 1, n_rows), col), (lax.rem(row + 1, n_rows), col)]


def torus_axes(n_rows, n_cols):
    row, col = lax.axis_index('row'), lax.axis_index('col')
    axes = [(n_cols, col, lambda d: (row, lax.rem(col + d, n_cols)))]
    for size, stride in row_digits(n_rows):
        place = lax.rem(row // stride, size)
        axes.append((size, place, functools.partial(
            lambda d, size, stride, place: (row + (lax.rem(place + d, size) - place) * stride, col),
            size=size, stride=stride, place=place)))
    return axes


def arrive(devices):
    for dev in devices:
        pl.semaphore_signal(pltpu.get_barrier_semaphore(), inc=1, device_id=dev, device_id_type=MESH)


def meet(devices):
    pl.semaphore_wait(pltpu.get_barrier_semaphore(), len(devices))


def start_exchange(peers, sbuf, rbuf, send_sem, recv_sem):
    copies = [remote(sbuf.at[q], rbuf.at[q ^ 1], send_sem.at[q], recv_sem.at[q ^ 1], peers[q]) for q in range(PEERS)]
    for copy in copies:
        copy.start()
    return copies


def axis_devices(axes):
    return [dev(d) for size, _, dev in axes for d in range(1, size)]


def exchange_kernel(n_rows, n_cols, sbuf, rbuf, send_sem, recv_sem):
    peers = grid_peers(n_rows, n_cols)
    arrive(peers)
    meet(peers)
    finish(start_exchange(peers, sbuf, rbuf, send_sem, recv_sem))


def first_kernel(n_rows, n_cols, xt, send_v, src_v, msk, rbuf, total_out, src4, sbuf, count, cv, cr,
                 send_sem, recv_sem, c_send, c_recv):
    peers, axes = grid_peers(n_rows, n_cols), torus_axes(n_rows, n_cols)
    everyone = peers + axis_devices(axes)
    arrive(everyone)
    n_feat, n_local = xt.shape
    halo = sbuf.shape[1]
    count[...] = jnp.full(count.shape, jnp.sum(msk[...].astype(F32)), F32)
    degree = src_v.shape[0]
    for b in range(n_local // LANES):
        src4[b, 0:degree, :] = src_v[:, b * LANES:(b + 1) * LANES] * 4
        src4[b, degree:, :] = jnp.zeros((src4.shape[1] - degree, LANES), jnp.int32)
    wanted = [jnp.transpose(jnp.broadcast_to(send_v[q:q + 1, :], (LANES, halo))) for q in range(PEERS)]
    wanted = jnp.concatenate([jnp.concatenate(wanted, axis=0)] * (BLOCK // LANES), axis=1)
    place = iota(wanted.shape, 1)

    def pick(blk, total):
        hot = (place == wanted - blk * BLOCK).astype(F32).astype(BF16)
        return total + lax.dot_general(hot, xt[:, block_rows(blk)], NT, preferred_element_type=F32)

    rows = lax.fori_loop(0, n_local // BLOCK, pick, jnp.zeros((PEERS * halo, n_feat), F32)).astype(BF16)
    for q in range(PEERS):
        sbuf[q, :, 0:n_feat] = rows[q * halo:(q + 1) * halo, :]
        sbuf[q, :, n_feat:] = jnp.zeros((halo, sbuf.shape[2] - n_feat), BF16)
    meet(everyone)
    copies = start_exchange(peers, sbuf, rbuf, send_sem, recv_sem)
    for i, (size, _, dev) in enumerate(axes):
        held = count if i == 0 else cv.at[i - 1]
        counts = [remote(held, cr.at[i, d - 1], c_send.at[i, d - 1], c_recv.at[i, d - 1], dev(d))
                  for d in range(1, size)]
        for copy in counts:
            copy.start()
        finish(counts)
        total = held[...]
        for d in range(1, size):
            total = total + cr[i, d - 1]
        cv[i] = total
    total_out[...] = cv[len(axes) - 1]
    finish(copies)


def reduce_over_devices(axes, ar, part, gb, rs, r_send, r_recv, g_send, g_recv):
    length, base, spans, at, offset, held = AR_ROWS, 0, [], 0, 0, ar
    for i, (size, place, dev) in enumerate(axes):
        length //= size
        copies = []
        for d in range(1, size):
            there = pl.multiple_of(lax.rem(place + d, size) * length, 8)
            copies.append(remote(held.at[pl.ds(there, length), :], rs.at[pl.ds(at + (d - 1) * length, length), :],
                                 r_send.at[i, d - 1], r_recv.at[i, d - 1], dev(d)))
        for copy in copies:
            copy.start()
        finish(copies)
        total = held[pl.ds(pl.multiple_of(place * length, 8), length), :]
        for d in range(1, size):
            total = total + rs[at + (d - 1) * length:at + d * length, :]
        part[offset:offset + length, :] = total
        held = part.at[pl.ds(offset, length), :]
        base = pl.multiple_of(base + place * length, 8)
        at += (size - 1) * length
        offset += length
        spans.append((base, length))
    gb[pl.ds(base, length), :] = held[...]
    for i in reversed(range(len(axes))):
        size, _, dev = axes[i]
        base, length = spans[i]
        here = gb.at[pl.ds(base, length), :]
        copies = [remote(here, here, g_send.at[i, d - 1], g_recv.at[i, d - 1], dev(d)) for d in range(1, size)]
        for copy in copies:
            copy.start()
        finish(copies)


def spread_weights(wt_v, wb):
    degree, n_local = wt_v.shape

    def spread(blk, _):
        for half in range(2):
            at = pl.ds(pl.multiple_of(blk * (2 * LANES) + half * LANES, LANES), LANES)
            for k in range(degree):
                wb[k, at, :] = jnp.transpose(jnp.broadcast_to(wt_v[k:k + 1, at], (LANES, LANES)))
        return 0

    lax.fori_loop(0, n_local // (2 * LANES), spread, 0)


def store_halo(table, n_local, rbuf):
    halo = rbuf.shape[1]
    for p in range(PEERS):
        for j in range(rbuf.shape[2] // LANES):
            table[pl.ds((n_local + p * halo) * 4 + j, halo, stride=4), :] = (
                rbuf[p, :, j * LANES:(j + 1) * LANES].astype(F32))


GROUP = 16


def gather_block(table, parts, src_s, wb, zb, blk):
    degree = wb.shape[0]

    def some(i, _):
        local = i * GROUP
        base = blk * BLOCK + local
        word = lax.shift_left(lax.shift_right_logical(base, 7), 10) + (base & (LANES - 1))
        for s in range(GROUP):
            total = None
            for k in range(degree):
                at = pl.multiple_of(src_s[word + (k * LANES + s)], 4)
                term = table[pl.ds(at, parts), :] * jnp.broadcast_to(wb[k, pl.ds(base + s, 1), :], (parts, LANES))
                total = term if total is None else total + term
            zb[pl.ds(pl.multiple_of((local + s) * parts, parts), parts), :] = total
        return 0

    lax.fori_loop(0, BLOCK // GROUP, some, 0)
    return jnp.concatenate([zb[pl.ds(j, BLOCK, stride=parts), :] for j in range(parts)], axis=1).astype(BF16)


def layer_one_kernel(src4, send_s, xt, wt_v, rbuf, w1, z1, h1, sbuf,
                     src_s, tab, tab2, wb, zb, w1b, z1_v, h1_v, sem):
    n_feat, n_local = xt.shape
    n_blocks = n_local // BLOCK
    halo = sbuf.shape[1]
    indices = pltpu.make_async_copy(src4, src_s, sem.at[0])
    indices.start()
    eye = (iota((BLOCK, BLOCK), 0) == iota((BLOCK, BLOCK), 1)).astype(F32).astype(BF16)

    def fill_table(blk, _):
        rows = lax.dot_general(eye, xt[:, block_rows(blk)], NT, preferred_element_type=F32)
        for j in range(4):
            part = rows[:, j * LANES:(j + 1) * LANES]
            if part.shape[1] < LANES:
                part = jnp.concatenate([part, jnp.zeros((BLOCK, LANES - part.shape[1]), F32)], axis=1)
            tab[pl.ds(blk * (4 * BLOCK) + j, BLOCK, stride=4), :] = part
        return 0

    lax.fori_loop(0, n_blocks, fill_table, 0)
    spread_weights(wt_v, wb)
    w1b[...] = jnp.zeros(w1b.shape, BF16)
    w1b[0:n_feat, :] = w1[...].astype(BF16)
    store_halo(tab, n_local, rbuf)
    indices.wait()

    def layer_one(blk, _):
        rows = block_rows(blk)
        z = gather_block(tab, 4, src_s, wb, zb, blk)
        z1_v[rows, :] = z
        h = jnp.maximum(jnp.dot(z, w1b[...], preferred_element_type=F32), 0.0).astype(BF16)
        h1_v[rows, :] = h
        pltpu.make_async_copy(z1_v.at[rows, :], z1.at[rows, :], sem.at[1]).start()
        pltpu.make_async_copy(h1_v.at[rows, :], h1.at[rows, :], sem.at[2]).start()
        for j in range(2):
            tab2[pl.ds(blk * (2 * BLOCK) + j, BLOCK, stride=2), :] = h[:, j * LANES:(j + 1) * LANES].astype(F32)
        return 0

    lax.fori_loop(0, n_blocks, layer_one, 0)

    for q in range(PEERS):
        def take(i, _):
            for s in range(16):
                r = i * 16 + s
                at = pl.multiple_of(send_s[q, r] * 2, 2)
                zb[pl.ds(pl.multiple_of(r * 2, 2), 2), :] = tab2[pl.ds(at, 2), :]
            return 0
        lax.fori_loop(0, halo // 16, take, 0)
        for j in range(2):
            sbuf[q, :, j * LANES:(j + 1) * LANES] = zb[pl.ds(j, halo, stride=2), :].astype(BF16)
    pltpu.make_async_copy(z1_v, z1, sem.at[1]).wait()
    pltpu.make_async_copy(h1_v, h1, sem.at[2]).wait()


def layer_two_kernel(src4, wt_v, h1, rbuf, w2t, z2, lg, src_s, tab, wb, zb, sem):
    n_class = w2t.shape[0]
    n_local = h1.shape[0]
    n_blocks = n_local // BLOCK
    indices = pltpu.make_async_copy(src4, src_s, sem)
    indices.start()

    def fill_table(blk, _):
        rows = h1[block_rows(blk), :].astype(F32)
        for j in range(2):
            tab[pl.ds(blk * (4 * BLOCK) + j, BLOCK, stride=4), :] = rows[:, j * LANES:(j + 1) * LANES]
        return 0

    lax.fori_loop(0, n_blocks, fill_table, 0)
    spread_weights(wt_v, wb)
    store_halo(tab, n_local, rbuf)
    w2p = jnp.concatenate([w2t[...], jnp.zeros((8 - n_class, w2t.shape[1]), F32)], axis=0).astype(BF16)
    indices.wait()

    def layer_two(blk, _):
        rows = block_rows(blk)
        z = gather_block(tab, 2, src_s, wb, zb, blk)
        z2[rows, :] = z
        lg[:, rows] = lax.dot_general(w2p, z, NT, preferred_element_type=F32)
        return 0

    lax.fori_loop(0, n_blocks, layer_two, 0)


def last_kernel(n_rows, n_cols, n_feat, src_v, wt_v, lab, msk, count, logit, z2, w2t, send_v, z1, h1,
                g1_out, g2_out, loss_out, z1_v, h1_v, lg, acc, g2t, hs, hr, ar, part_sum, gb, rs,
                sem, send_sem, recv_sem, r_send, r_recv, g_send, g_recv):
    peers, axes = grid_peers(n_rows, n_cols), torus_axes(n_rows, n_cols)
    everyone = peers + axis_devices(axes)
    arrive(everyone)
    z1_load = pltpu.make_async_copy(z1, z1_v, sem.at[0])
    h1_load = pltpu.make_async_copy(h1, h1_v, sem.at[1])
    z1_load.start()
    h1_load.start()
    degree, n_local = src_v.shape
    n_class = w2t.shape[0]
    n_blocks = n_local // BLOCK
    halo = hs.shape[2]
    half = AR_ROWS // 2

    logits = logit[...]
    cls = iota(logits.shape, 0)
    real = cls < n_class
    top = jnp.max(jnp.where(real, logits, jnp.finfo(F32).min), axis=0, keepdims=True)
    log_norm = top + jnp.log(jnp.sum(jnp.where(real, jnp.exp(logits - top), 0.0), axis=0, keepdims=True))
    onehot = (cls == lab[...]).astype(F32)
    picked = jnp.sum(onehot * logits, axis=0, keepdims=True)
    weight = msk[...].astype(F32)
    loss_sum = jnp.sum(weight * (log_norm - picked), axis=1, keepdims=True)
    prob = jnp.where(real, jnp.exp(logits - log_norm), 0.0)
    lg[...] = (prob - onehot) * (weight / count[0:1, 0:1])

    spread_cls = spread_classes(n_class)
    lc_blk = block_of_unit((LANES, BLOCK))
    slot = iota((BLOCK, BLOCK), 0)
    acc[...] = jnp.zeros(acc.shape, F32)
    g2t[...] = jnp.zeros(g2t.shape, F32)

    def scatter(blk, _):
        cols = block_rows(blk)
        g = lg[:, cols].astype(BF16)
        g2t[...] += jnp.dot(g, z2[cols, :], preferred_element_type=F32)
        tiled = jnp.dot(spread_cls, g, preferred_element_type=F32)
        total = acc[...]
        for k in range(degree):
            src = src_v[k:k + 1, cols]
            left = jnp.where(lax.shift_right_logical(src, 8) == lc_blk, tiled, 0.0).astype(BF16)
            here = (src & (BLOCK - 1)) == slot
            for part in pieces(wt_v[k:k + 1, cols]):
                right = jnp.where(here, part.astype(F32), 0.0).astype(BF16)
                total = total + lax.dot_general(left, right, NT, preferred_element_type=F32)
        acc[...] = total
        return 0

    lax.fori_loop(0, n_blocks, scatter, 0)

    hs[...] = jnp.zeros(hs.shape, F32)
    for p in range(PEERS):
        first = (n_local + p * halo) // BLOCK * n_class
        lane = (n_local + p * halo) % BLOCK
        hs[p, 0:n_class, :] = acc[first:first + n_class, lane:lane + halo]
    meet(everyone)
    copies = start_exchange(peers, hs, hr, send_sem, recv_sem)

    w2p = jnp.concatenate([w2t[...], jnp.zeros((8 - n_class, w2t.shape[1]), F32)], axis=0).astype(BF16)
    w2_tiled = jnp.dot(spread_cls, w2p, preferred_element_type=F32)
    ar[...] = jnp.zeros(ar.shape, F32)
    dst = send_v[...]
    wide = dst.shape[1]
    dst_blk = lax.shift_right_logical(dst, 8) == block_of_unit((LANES, wide))
    right = ((dst & (BLOCK - 1)) == iota((BLOCK, wide), 0)).astype(F32).astype(BF16)
    z1_load.wait()
    h1_load.wait()
    finish(copies)

    total = acc[...]
    returned = jnp.concatenate([hr[q] for q in range(PEERS)], axis=1)
    for part in pieces(returned):
        tiled = jnp.dot(spread_cls, part, preferred_element_type=F32)
        left = jnp.where(dst_blk, tiled, 0.0).astype(BF16)
        total = total + lax.dot_general(left, right, NT, preferred_element_type=F32)
    turned = jnp.concatenate(pieces(jnp.transpose(total)), axis=1)

    def weight_grad(blk, _):
        rows = block_rows(blk)
        w2_here = jnp.where(lc_blk == blk, w2_tiled, 0.0).astype(BF16)
        dh = jnp.dot(turned, jnp.concatenate([w2_here] * 3, axis=0), preferred_element_type=F32)
        d_one = jnp.where(h1_v[rows, :].astype(F32) > 0, dh, 0.0).astype(BF16)
        grad = lax.dot_general(z1_v[rows, :], d_one, TN, preferred_element_type=F32)
        ar[0:half, :] += grad[:, :LANES]
        ar[half:2 * half, :] += grad[:, LANES:]
        return 0

    lax.fori_loop(0, n_blocks, weight_grad, 0)
    for j in range(2):
        ar[j * half + n_feat:j * half + n_feat + n_class, :] = g2t[0:n_class, j * LANES:(j + 1) * LANES]
    ar[n_feat + n_class:n_feat + n_class + 1, :] = jnp.broadcast_to(loss_sum, (1, LANES))

    reduce_over_devices(axes, ar, part_sum, gb, rs, r_send, r_recv, g_send, g_recv)
    for j in range(2):
        lanes = slice(j * LANES, (j + 1) * LANES)
        g1_out[:, lanes] = gb[j * half:j * half + n_feat, :]
        g2_out[:, lanes] = gb[j * half + n_feat:j * half + n_feat + n_class, :]
    loss_out[...] = gb[n_feat + n_class:n_feat + n_class + 1, :] / count[0:1, :]


def call(kernel, name, outs, in_specs, out_specs, scratch, args, collective=None):
    params = dict(vmem_limit_bytes=60 * 1024 * 1024)
    if collective is not None:
        params.update(collective_id=collective, has_side_effects=True)
    shapes = tuple(jax.ShapeDtypeStruct(*o) for o in outs)
    return pl.pallas_call(kernel, out_shape=shapes, in_specs=in_specs, out_specs=tuple(out_specs),
                          scratch_shapes=scratch, compiler_params=pltpu.CompilerParams(**params), name=name)(*args)


def solution(mesh):
    n_rows = mesh.shape['row']
    n_cols = mesh.shape['col']
    grid_axes = ('row', 'col')

    def device_step(node_feat, w_one, w_two, send_rows, edge_src, edge_wt, labels, label_mask):
        n_local, n_feat = node_feat.shape
        hidden, n_class = w_two.shape
        halo = send_rows.shape[1]
        degree = edge_src.shape[1]
        ext = n_local + PEERS * halo
        sizes = [n_cols] + [s for s, _ in row_digits(n_rows)]
        n_axes = len(sizes)
        dma, vm = pltpu.SemaphoreType.DMA, pltpu.VMEM
        feat_pad = 4 * LANES
        xt, src_v, wt_v, w2t = node_feat.T, edge_src.T, edge_wt.T, w_two.T
        lab, msk = labels.reshape(1, -1), label_mask.reshape(1, -1)

        rbuf, count, src4 = call(
            functools.partial(first_kernel, n_rows, n_cols), 'first',
            [((PEERS, halo, feat_pad), BF16), ((8, LANES), F32), ((n_local // LANES, 8, LANES), jnp.int32)],
            [VMEM] * 4, [VMEM] * 3,
            [vm((PEERS, halo, feat_pad), BF16), vm((8, LANES), F32),
             vm((n_axes, 8, LANES), F32), vm((n_axes, 3, 8, LANES), F32),
             dma((PEERS,)), dma((PEERS,)), dma((n_axes, 3)), dma((n_axes, 3))], (xt, send_rows, src_v, msk), 0)
        src4 = src4.reshape(-1)
        z1, h1, sbuf2 = call(
            layer_one_kernel, 'layer_one',
            [((n_local, feat_pad), BF16), ((n_local, hidden), BF16), ((PEERS, halo, hidden), BF16)],
            [ANY, SMEM] + [VMEM] * 4, [ANY, ANY, VMEM],
            [pltpu.SMEM((8 * n_local,), jnp.int32), vm((ext * 4, LANES), F32), vm((n_local * 2, LANES), F32),
             vm((degree, n_local, LANES), F32), vm((BLOCK * 4, LANES), F32), vm((feat_pad, hidden), BF16),
             vm((n_local, feat_pad), BF16), vm((n_local, hidden), BF16), dma((3,))],
            (src4, send_rows, xt, wt_v, rbuf, w_one))
        rbuf2, = call(functools.partial(exchange_kernel, n_rows, n_cols), 'exchange_hidden',
                      [((PEERS, halo, hidden), BF16)], [VMEM], [VMEM], [dma((PEERS,)), dma((PEERS,))], (sbuf2,), 1)
        z2, logit = call(
            layer_two_kernel, 'layer_two', [((n_local, hidden), BF16), ((8, n_local), F32)],
            [ANY] + [VMEM] * 4, [VMEM] * 2,
            [pltpu.SMEM((8 * n_local,), jnp.int32), vm((ext * 4, LANES), F32), vm((degree, n_local, LANES), F32),
             vm((BLOCK * 2, LANES), F32), dma(())],
            (src4, wt_v, h1, rbuf2, w2t))
        part_rows, rs_rows, left = 0, 0, AR_ROWS
        for size in sizes:
            left //= size
            part_rows += left
            rs_rows += (size - 1) * left
        g1, g2, total = call(
            functools.partial(last_kernel, n_rows, n_cols, n_feat), 'last',
            [((n_feat, hidden), F32), ((n_class, hidden), F32), ((1, LANES), F32)],
            [VMEM] * 9 + [ANY] * 2, [VMEM] * 3,
            [vm((n_local, feat_pad), BF16), vm((n_local, hidden), BF16), vm((8, n_local), F32),
             vm((LANES, BLOCK), F32), vm((8, hidden), F32), vm((PEERS, 8, halo), F32), vm((PEERS, 8, halo), F32),
             vm((AR_ROWS, LANES), F32), vm((part_rows, LANES), F32), vm((AR_ROWS, LANES), F32),
             vm((rs_rows, LANES), F32), dma((2,)), dma((PEERS,)), dma((PEERS,)),
             dma((n_axes, 3)), dma((n_axes, 3)), dma((n_axes, 3)), dma((n_axes, 3))],
            (src_v, wt_v, lab, msk, count, logit, z2, w2t, send_rows.reshape(1, -1), z1, h1), 2)
        return total[0, 0], g1, g2.T

    rows_spec = P(grid_axes, None)
    vec_spec = P(grid_axes)
    return jax.shard_map(device_step, mesh=mesh,
                         in_specs=(rows_spec, P(), P(), rows_spec, rows_spec, rows_spec, vec_spec, vec_spec),
                         out_specs=(P(), P(), P()), check_vma=False)
```
